32 devices in a mesh: rows: 32 (over z, y, x, core).
Axes of the slice: x: 2, y: 2, z: 4, core: 2. Of those that a mesh axis runs over, the one named last changes fastest.
Arguments:
- adj_diag: int32 [512, 512], P('rows'), may hold values from -2147483648 to 2147483647
- adj_right: int32 [512, 512], P('rows'), may hold values from -2147483648 to 2147483647
- alive_diag: int32 [512, 512], P('rows'), may hold values from -2147483648 to 2147483647
- alive_right: int32 [512, 512], P('rows'), may hold values from -2147483648 to 2147483647
- truss_k: int32 [1], replicated, may hold values from 130 to 193
Outputs:
- support_field: float32 [16384, 1024], P('rows')
- removed_counts: int32 [3], replicated
The draws below stay inside these ranges and needn't reach their ends.
All inputs are finite; a program needn't handle non-finite values.
Results may differ from the reference program's by a relative error of at most 0.0003.
Values may be sent and summed in bfloat16 or wider, within the bound.
A program may use at most 64 MiB of HBM per device.

```python
import jax
import jax.numpy as jnp
from jax import lax

TILE = 512
ITERS = 3
NVERT = 16384


def vertex_levels(key, block):
    base_key = jax.random.fold_in(jax.random.fold_in(key, 7001), block)
    size_key, order_key, level_key = jax.random.split(base_key, 3)
    core_count = jax.random.randint(size_key, (), TILE // 4, 3 * TILE // 8 + 1, dtype=jnp.int32)
    order = jax.random.permutation(order_key, TILE)
    is_core = order < core_count
    levels = jax.random.randint(level_key, (TILE,), 2, 16, dtype=jnp.int32)
    return (jnp.where(is_core, jnp.int32(16), levels), is_core)


def pack_bits(tile_bits):
    shifts = jnp.arange(32, dtype=jnp.int32)
    sectioned = tile_bits.reshape(TILE // 32, 32, TILE)
    return jnp.sum(sectioned << shifts[None, :, None], axis=1, dtype=jnp.int32)


def draw_bits(key, salt, offset, alive_kind):
    blocks = NVERT // TILE

    def one_block(block):
        row_levels, row_core = vertex_levels(key, block)
        col_levels, col_core = vertex_levels(key, (block + offset) % blocks)
        edge_key = jax.random.fold_in(jax.random.fold_in(key, salt), block)
        if alive_kind:
            chance = jax.random.randint(edge_key, (TILE, TILE), 0, 8, dtype=jnp.int32)
            both_core = row_core[:, None] & col_core[None, :]
            tile_bits = jnp.where(both_core, jnp.int32(1), (chance < 7).astype(jnp.int32))
        else:
            chance = jax.random.randint(edge_key, (TILE, TILE), 0, 256, dtype=jnp.int32)
            tile_bits = (chance < row_levels[:, None] * col_levels[None, :]).astype(jnp.int32)
        return pack_bits(tile_bits)
    packed = lax.map(one_block, jnp.arange(blocks, dtype=jnp.int32))
    return packed.reshape(NVERT // 32, TILE)


def draw_adj_diag(key, part):
    return draw_bits(key, 101, 0, False)


def draw_adj_right(key, part):
    return draw_bits(key, 102, 1, False)


def draw_alive_diag(key, part):
    return draw_bits(key, 103, 0, True)


def draw_alive_right(key, part):
    return draw_bits(key, 104, 1, True)


def setup_inputs(seed: int = 0) -> dict:
    seeds = jax.random.split(jax.random.key(seed), 6)
    adj_diag = draw_adj_diag(jax.random.fold_in(seeds[5], 71), 0)
    adj_right = draw_adj_right(jax.random.fold_in(seeds[5], 71), 0)
    alive_diag = draw_alive_diag(jax.random.fold_in(seeds[5], 71), 0)
    alive_right = draw_alive_right(jax.random.fold_in(seeds[5], 71), 0)
    truss_k = jax.random.randint(seeds[4], (1,), TILE // 4 + 2, 3 * TILE // 8 + 2).astype(jnp.int32)
    return {"adj_diag": adj_diag, "adj_right": adj_right, "alive_diag": alive_diag, "alive_right": alive_right, "truss_k": truss_k}


def unpack_tiles(packed, blocks, tile):
    shifts = jnp.arange(32, dtype=jnp.int32)
    sectioned = packed.reshape(blocks, tile // 32, tile)
    tile_bits = (sectioned[:, :, None, :] >> shifts[None, None, :, None]) & 1
    return tile_bits.reshape(blocks, tile, tile)


def tile_support(pieces):
    within, across, prev_across, next_within = pieces
    inside = lax.dot_general(prev_across, prev_across, (((0,), (0,)), ((), ())), preferred_element_type=jnp.float32)
    inside = inside + jnp.dot(within, within, preferred_element_type=jnp.float32)
    inside = inside + lax.dot_general(across, across, (((1,), (1,)), ((), ())), preferred_element_type=jnp.float32)
    between = jnp.dot(within, across, preferred_element_type=jnp.float32)
    between = between + jnp.dot(across, next_within, preferred_element_type=jnp.float32)
    return inside, between


def reference(adj_diag, adj_right, alive_diag, alive_right, truss_k):
    blocks = NVERT // TILE
    upper_half = jnp.triu(unpack_tiles(adj_diag & alive_diag, blocks, TILE), 1)
    within = (upper_half + jnp.swapaxes(upper_half, 1, 2)).astype(jnp.bfloat16)
    across = unpack_tiles(adj_right & alive_right, blocks, TILE).astype(jnp.bfloat16)
    thresh = (truss_k[0] - 2).astype(jnp.float32)
    counts = []
    for step in range(ITERS):
        prev_across = jnp.roll(across, 1, axis=0)
        next_within = jnp.roll(within, -1, axis=0)
        inside, between = lax.map(tile_support, (within, across, prev_across, next_within))
        new_within = jnp.where(inside >= thresh, within, jnp.zeros_like(within))
        new_across = jnp.where(between >= thresh, across, jnp.zeros_like(across))
        lost_within = jnp.sum((within - new_within).astype(jnp.int32)) // 2
        lost_across = jnp.sum((across - new_across).astype(jnp.int32))
        counts.append(lost_within + lost_across)
        within, across = new_within, new_across
    support = jnp.concatenate([inside * within.astype(jnp.float32), between * across.astype(jnp.float32)], axis=2)
    return support.reshape(NVERT, 2 * TILE), jnp.stack(counts).astype(jnp.int32)
```

```python
import functools

import jax
import jax.numpy as jnp
from jax import lax
from jax.experimental import pallas as pl
from jax.experimental.pallas import tpu as pltpu
from jax.sharding import PartitionSpec as P

F8 = jnp.float8_e4m3fn
F32 = jnp.float32
WORD = 32


def dot_nt(lhs, rhs):
    return lax.dot_general(lhs, rhs, (((1,), (1,)), ((), ())), preferred_element_type=F32)


def send(src, dst, send_sem, recv_sem, target):
    return pltpu.make_async_remote_copy(
        src_ref=src,
        dst_ref=dst,
        send_sem=send_sem,
        recv_sem=recv_sem,
        device_id=(target,),
        device_id_type=pl.DeviceIdType.MESH,
    )


def kernel(
    n, k_ref, ad_ref, ar_ref, ld_ref, lr_ref, out_ref, cnt_ref,
    own, halo, x, eye, tri, psum_in, psum_next, psum_btw, mine, gathered,
    send_sems, recv_sems, cnt_send, cnt_recv,
):
    t = ad_ref.shape[1]
    words = ad_ref.shape[0]
    me = lax.axis_index("rows")
    barrier = pltpu.get_barrier_semaphore()

    def greet(d, carry):
        pl.semaphore_signal(
            barrier, inc=1, device_id=(lax.rem(me + d, n),), device_id_type=pl.DeviceIdType.MESH
        )
        return carry

    lax.fori_loop(1, n, greet, 0)
    own[0] = ad_ref[...] & ld_ref[...]
    own[1] = ar_ref[...] & lr_ref[...]

    AT, W, A = (pl.ds(i * t, t) for i in range(3))
    shift = lax.broadcasted_iota(jnp.int32, (WORD, t), 0)
    col = lax.broadcasted_iota(jnp.int32, (WORD, t), 1)

    def unpack(src, upper):
        dst = []
        for w in range(words):
            bits = (jnp.broadcast_to(src[w : w + 1, :], (WORD, t)) >> shift) & 1
            if upper:
                bits = jnp.where(col - shift > WORD * w, bits, 0)
            dst.append(bits.astype(F32).astype(F8))
        return dst

    def put_across(src, j):
        for w, rows in enumerate(unpack(src, False)):
            x[j, pl.ds(WORD * w, WORD), A] = rows

    def put_transposed(j):
        x[j + 1, :, AT] = dot_nt(eye[...], x[j, :, A]).astype(F8)

    def put_within(src, j):
        for w, rows in enumerate(unpack(src, True)):
            tri[pl.ds(WORD * w, WORD), :] = rows
        flipped = dot_nt(eye[...], tri[...])
        x[j, :, W] = (flipped + tri[...].astype(F32)).astype(F8)

    row_id = lax.broadcasted_iota(jnp.int32, (t, t), 0)
    col_id = lax.broadcasted_iota(jnp.int32, (t, t), 1)
    eye[...] = jnp.where(row_id == col_id, 1.0, 0.0).astype(F32).astype(F8)
    put_across(own.at[1], 1)

    pl.semaphore_wait(barrier, n - 1)
    routes = ((1, 2, 1), (0, 1, 1), (0, 3, -1), (1, 4, -1), (1, 0, 2), (0, 5, -2))
    copies = {}
    for what, slot, by in routes:
        copies[slot] = send(
            own.at[what], halo.at[slot], send_sems.at[slot], recv_sems.at[slot],
            lax.rem(me + by + n, n),
        )
        copies[slot].start()

    thresh = (k_ref[0] - 2).astype(F32)

    put_within(own.at[0], 1)
    put_transposed(1)
    psum_in[...] = dot_nt(x[1, :, t:], x[1, :, t:])
    psum_next[...] = dot_nt(x[2, :, AT], x[2, :, AT])
    psum_btw[...] = dot_nt(x[1, :, W], x[2, :, AT])

    def total(values):
        lanes = jnp.sum(values, axis=0, keepdims=True)
        return sum(lanes[:, i : i + 128] for i in range(0, t, 128))

    def keep(support, j, part):
        old = x[j, :, part].astype(F32)
        return old, jnp.where(support >= thresh, old, 0.0)

    def inside(j):
        return dot_nt(x[j], x[j])

    def between(j):
        return dot_nt(x[j, :, t:], x[j + 1, :, : 2 * t])

    copies[2].wait_recv()
    put_across(halo.at[2], 0)
    put_transposed(0)
    copies[1].wait_recv()
    put_within(halo.at[1], 0)
    copies[3].wait_recv()
    put_within(halo.at[3], 2)
    copies[4].wait_recv()
    put_across(halo.at[4], 2)
    put_transposed(2)
    copies[0].wait_recv()
    for w, rows in enumerate(unpack(halo.at[0], False)):
        tri[pl.ds(WORD * w, WORD), :] = rows
    x[0, :, AT] = dot_nt(eye[...], tri[...]).astype(F8)
    copies[5].wait_recv()
    put_within(halo.at[5], 3)

    counts = []

    def own_count(old_w, new_w, old_a, new_a):
        counts.append(total((old_w - new_w) + 2.0 * (old_a - new_a)))

    _, wm = keep(inside(0), 0, W)
    _, am = keep(between(0), 0, A)
    old_w, w0 = keep(psum_in[...] + dot_nt(x[1, :, AT], x[1, :, AT]), 1, W)
    old_a, a0 = keep(psum_btw[...] + dot_nt(x[1, :, A], x[2, :, W]), 1, A)
    own_count(old_w, w0, old_a, a0)
    _, w1 = keep(psum_next[...] + dot_nt(x[2, :, t:], x[2, :, t:]), 2, W)
    _, a1 = keep(between(2), 2, A)
    x[0, :, W] = wm.astype(F8)
    x[0, :, A] = am.astype(F8)
    x[1, :, W] = w0.astype(F8)
    x[1, :, A] = a0.astype(F8)
    x[2, :, W] = w1.astype(F8)
    x[2, :, A] = a1.astype(F8)
    put_transposed(0)
    put_transposed(1)

    _, am = keep(between(0), 0, A)
    old_w, w0 = keep(inside(1), 1, W)
    old_a, a0 = keep(between(1), 1, A)
    own_count(old_w, w0, old_a, a0)
    _, w1 = keep(inside(2), 2, W)
    x[0, :, A] = am.astype(F8)
    x[1, :, W] = w0.astype(F8)
    x[1, :, A] = a0.astype(F8)
    x[2, :, W] = w1.astype(F8)
    put_transposed(0)
    put_transposed(1)

    support_w = inside(1)
    old_w, w0 = keep(support_w, 1, W)
    support_a = between(1)
    old_a, a0 = keep(support_a, 1, A)
    own_count(old_w, w0, old_a, a0)
    mine[...] = jnp.zeros_like(mine)
    for step, row in enumerate(counts):
        mine[step : step + 1, :] = row.astype(jnp.int32)

    def share(d, carry):
        send(mine, gathered.at[d - 1], cnt_send, cnt_recv, lax.rem(me + d, n)).start()
        return carry

    lax.fori_loop(1, n, share, 0)
    out_ref[:, :t] = support_w * w0
    out_ref[:, t:] = support_a * a0
    for slot in range(6):
        copies[slot].wait_send()
    pltpu.make_async_copy(gathered, gathered, cnt_recv).wait()
    summed = mine[...] + jnp.sum(gathered[...], axis=0)
    for step in range(cnt_ref.shape[0]):
        cnt_ref[step] = jnp.sum(summed[step : step + 1, :]) // 2
    pltpu.make_async_copy(gathered, gathered, cnt_send).wait()


def on_device(n, adj_diag, adj_right, alive_diag, alive_right, truss_k):
    words, t = adj_diag.shape
    vmem = pl.BlockSpec(memory_space=pltpu.VMEM)
    smem = pl.BlockSpec(memory_space=pltpu.SMEM)
    return pl.pallas_call(
        functools.partial(kernel, n),
        out_shape=(
            jax.ShapeDtypeStruct((t, 2 * t), F32),
            jax.ShapeDtypeStruct((3,), jnp.int32),
        ),
        in_specs=[smem] + [vmem] * 4,
        out_specs=(vmem, smem),
        scratch_shapes=[
            pltpu.VMEM((2, words, t), jnp.int32),
            pltpu.VMEM((6, words, t), jnp.int32),
            pltpu.VMEM((4, t, 3 * t), F8),
            pltpu.VMEM((t, t), F8),
            pltpu.VMEM((t, t), F8),
            pltpu.VMEM((t, t), F32),
            pltpu.VMEM((t, t), F32),
            pltpu.VMEM((t, t), F32),
            pltpu.VMEM((8, 128), jnp.int32),
            pltpu.VMEM((n - 1, 8, 128), jnp.int32),
            pltpu.SemaphoreType.DMA((6,)),
            pltpu.SemaphoreType.DMA((6,)),
            pltpu.SemaphoreType.DMA,
            pltpu.SemaphoreType.DMA,
        ],
        compiler_params=pltpu.CompilerParams(collective_id=0, has_side_effects=True),
    )(truss_k, adj_diag, adj_right, alive_diag, alive_right)


def solution(mesh):
    row = P("rows", None)
    return jax.shard_map(
        functools.partial(on_device, mesh.shape["rows"]),
        mesh=mesh,
        in_specs=(row, row, row, row, P()),
        out_specs=(row, P()),
        check_vma=False,
    )
```

```python
import functools

import jax
import jax.numpy as jnp
from jax import lax
from jax.experimental import pallas as pl
from jax.experimental.pallas import tpu as pltpu
from jax.sharding import PartitionSpec as P

F8 = jnp.float8_e4m3fn
F32 = jnp.float32
WORD = 32


def dot_nt(lhs, rhs):
    return lax.dot_general(lhs, rhs, (((1,), (1,)), ((), ())), preferred_element_type=F32)


def send(src, dst, send_sem, recv_sem, target):
    return pltpu.make_async_remote_copy(
        src_ref=src,
        dst_ref=dst,
        send_sem=send_sem,
        recv_sem=recv_sem,
        device_id=(target,),
        device_id_type=pl.DeviceIdType.MESH,
    )


def kernel(
    n, k_ref, ad_ref, ar_ref, ld_ref, lr_ref, out_ref, cnt_ref,
    raw, own, halo, x, eye, tri, spare, psum_in, psum_next, psum_btw, mine, gathered,
    raw_sems, send_sems, recv_sems, relay_sems, cnt_send, cnt_recv,
):
    t = ad_ref.shape[1]
    words = ad_ref.shape[0]
    me = lax.axis_index("rows")
    even = lax.rem(me, 2) == 0
    loads = [
        pltpu.make_async_copy(src, raw.at[i], raw_sems.at[i])
        for i, src in enumerate((ad_ref, ar_ref, ld_ref, lr_ref))
    ]
    for load in loads:
        load.start()
    barrier = pltpu.get_barrier_semaphore()

    def greet(d, carry):
        pl.semaphore_signal(
            barrier, inc=1, device_id=(lax.rem(me + d, n),), device_id_type=pl.DeviceIdType.MESH
        )
        return carry

    lax.fori_loop(1, n, greet, 0)
    for load in loads:
        load.wait()
    own[0] = raw[0] & raw[2]
    own[1] = raw[1] & raw[3]

    AT, W, A = (pl.ds(i * t, t) for i in range(3))
    shift = lax.broadcasted_iota(jnp.int32, (WORD, t), 0)
    col = lax.broadcasted_iota(jnp.int32, (WORD, t), 1)

    half = t // 2

    def unpack(src, upper):
        for w in range(words):
            left = half if upper and 2 * w >= words else 0
            bits = (jnp.broadcast_to(src[w : w + 1, left:], (WORD, t - left)) >> shift[:, left:]) & 1
            if upper:
                bits = jnp.where(col[:, left:] - shift[:, left:] > WORD * w, bits, 0)
            yield pl.ds(WORD * w, WORD), pl.ds(left, t - left), bits.astype(F32).astype(F8)

    def put_across(src, j):
        for rows, _, bits in unpack(src, False):
            x[j, rows, A] = bits

    def put_transposed(j):
        x[j + 1, :, AT] = dot_nt(eye[...], x[j, :, A]).astype(F8)

    def put_within(src, j):
        for rows, cols, bits in unpack(src, True):
            tri[rows, cols] = bits
        flipped = dot_nt(eye[...], tri[...])
        x[j, :, W] = (flipped + tri[...].astype(F32)).astype(F8)

    row_id = lax.broadcasted_iota(jnp.int32, (t, t), 0)
    col_id = lax.broadcasted_iota(jnp.int32, (t, t), 1)
    eye[...] = jnp.where(row_id == col_id, 1.0, 0.0).astype(F32).astype(F8)
    tri[half:, :half] = jnp.zeros((t - half, half), F32).astype(F8)
    put_across(own.at[1], 1)

    pl.semaphore_wait(barrier, n - 1)
    top, low = pl.ds(0, words // 2), pl.ds(words // 2, words // 2)
    whole, right = pl.ds(0, t), pl.ds(half, half)

    def pieces(source, slot, by, sends):
        parts = [(top, whole), (low, right if slot in (1, 3, 5) else whole)]
        return [
            send(
                source.at[rows, cols], halo.at[slot, rows, cols],
                sends.at[i], recv_sems.at[2 * slot + i], lax.rem(me + by + n, n),
            )
            for i, (rows, cols) in enumerate(parts)
        ]

    def start(slot):
        for piece in copies[slot]:
            piece.start()

    def arrive(slot):
        for piece in copies[slot]:
            piece.wait_recv()

    def left(copy):
        for piece in copy:
            piece.wait_send()

    routes = {2: (1, 1), 3: (0, -1), 1: (0, 1), 4: (1, -1), 0: (1, 2), 5: (0, -2)}
    copies = {
        slot: pieces(own.at[what], slot, by, send_sems.at[slot])
        for slot, (what, by) in routes.items()
    }
    to_right = pieces(halo.at[2], 0, 1, relay_sems)
    to_left = pieces(halo.at[3], 5, -1, relay_sems)
    start(2)
    start(3)

    @pl.when(even)
    def _():
        start(0)

    @pl.when(jnp.logical_not(even))
    def _():
        start(5)

    start(1)
    start(4)

    thresh = (k_ref[0] - 2).astype(F32)

    put_within(own.at[0], 1)
    put_transposed(1)
    psum_in[...] = dot_nt(x[1, :, t:], x[1, :, t:])
    psum_next[...] = dot_nt(x[2, :, AT], x[2, :, AT])
    psum_btw[...] = dot_nt(x[1, :, W], x[2, :, AT])

    def total(values):
        lanes = jnp.sum(values, axis=0, keepdims=True)
        return sum(lanes[:, i : i + 128] for i in range(0, t, 128))

    def keep(support, j, part):
        old = x[j, :, part].astype(F32)
        return old, jnp.where(support >= thresh, old, 0.0)

    def inside(j):
        return dot_nt(x[j], x[j])

    def between(j):
        return dot_nt(x[j, :, t:], x[j + 1, :, : 2 * t])

    arrive(2)

    @pl.when(even)
    def _():
        for piece in to_right:
            piece.start()

    arrive(3)

    @pl.when(jnp.logical_not(even))
    def _():
        for piece in to_left:
            piece.start()

    put_across(halo.at[2], 0)
    put_transposed(0)
    put_within(halo.at[3], 2)

    counts = []

    def own_count(old_w, new_w, old_a, new_a):
        counts.append(total((old_w - new_w) + 2.0 * (old_a - new_a)))

    old_w, w0 = keep(psum_in[...] + dot_nt(x[1, :, AT], x[1, :, AT]), 1, W)
    old_a, a0 = keep(psum_btw[...] + dot_nt(x[1, :, A], x[2, :, W]), 1, A)
    own_count(old_w, w0, old_a, a0)
    arrive(1)
    put_within(halo.at[1], 0)
    arrive(4)
    put_across(halo.at[4], 2)
    put_transposed(2)
    _, am = keep(between(0), 0, A)
    _, w1 = keep(psum_next[...] + dot_nt(x[2, :, t:], x[2, :, t:]), 2, W)
    arrive(0)
    for rows, _, bits in unpack(halo.at[0], False):
        spare[rows, :] = bits
    x[0, :, AT] = dot_nt(eye[...], spare[...]).astype(F8)
    _, wm = keep(inside(0), 0, W)
    arrive(5)
    put_within(halo.at[5], 3)
    _, a1 = keep(between(2), 2, A)
    x[0, :, W] = wm.astype(F8)
    x[0, :, A] = am.astype(F8)
    x[1, :, W] = w0.astype(F8)
    x[1, :, A] = a0.astype(F8)
    x[2, :, W] = w1.astype(F8)
    x[2, :, A] = a1.astype(F8)
    put_transposed(0)
    put_transposed(1)

    _, am = keep(between(0), 0, A)
    old_w, w0 = keep(inside(1), 1, W)
    old_a, a0 = keep(between(1), 1, A)
    own_count(old_w, w0, old_a, a0)
    _, w1 = keep(inside(2), 2, W)
    x[0, :, A] = am.astype(F8)
    x[1, :, W] = w0.astype(F8)
    x[1, :, A] = a0.astype(F8)
    x[2, :, W] = w1.astype(F8)
    put_transposed(0)
    put_transposed(1)

    support_w = inside(1)
    old_w, w0 = keep(support_w, 1, W)
    support_a = between(1)
    old_a, a0 = keep(support_a, 1, A)
    own_count(old_w, w0, old_a, a0)
    lane = lax.broadcasted_iota(jnp.int32, (1, 128), 1)
    packed = jnp.zeros((1, 128), F32)
    for step, row in enumerate(counts):
        packed = jnp.where(lane == step, jnp.sum(row, axis=1, keepdims=True), packed)
    mine[...] = packed.astype(jnp.int32)

    def share(d, carry):
        send(mine, gathered.at[d - 1], cnt_send, cnt_recv, lax.rem(me + d, n)).start()
        return carry

    lax.fori_loop(1, n, share, 0)
    out_ref[:, :t] = support_w * w0
    out_ref[:, t:] = support_a * a0
    for slot in range(1, 5):
        left(copies[slot])

    @pl.when(even)
    def _():
        left(copies[0])
        left(to_right)

    @pl.when(jnp.logical_not(even))
    def _():
        left(copies[5])
        left(to_left)

    pltpu.make_async_copy(gathered, gathered, cnt_recv).wait()
    summed = mine[...] + jnp.sum(gathered[...], axis=0)
    for step in range(cnt_ref.shape[0]):
        cnt_ref[step] = jnp.sum(jnp.where(lane == step, summed, 0)) // 2
    pltpu.make_async_copy(gathered, gathered, cnt_send).wait()


def on_device(n, adj_diag, adj_right, alive_diag, alive_right, truss_k):
    words, t = adj_diag.shape
    vmem = pl.BlockSpec(memory_space=pltpu.VMEM)
    smem = pl.BlockSpec(memory_space=pltpu.SMEM)
    return pl.pallas_call(
        functools.partial(kernel, n),
        out_shape=(
            jax.ShapeDtypeStruct((t, 2 * t), F32),
            jax.ShapeDtypeStruct((3,), jnp.int32),
        ),
        in_specs=[smem] + [pl.BlockSpec(memory_space=pltpu.MemorySpace.HBM)] * 4,
        out_specs=(vmem, smem),
        scratch_shapes=[
            pltpu.VMEM((4, words, t), jnp.int32),
            pltpu.VMEM((2, words, t), jnp.int32),
            pltpu.VMEM((6, words, t), jnp.int32),
            pltpu.VMEM((4, t, 3 * t), F8),
            pltpu.VMEM((t, t), F8),
            pltpu.VMEM((t, t), F8),
            pltpu.VMEM((t, t), F8),
            pltpu.VMEM((t, t), F32),
            pltpu.VMEM((t, t), F32),
            pltpu.VMEM((t, t), F32),
            pltpu.VMEM((1, 128), jnp.int32),
            pltpu.VMEM((n - 1, 1, 128), jnp.int32),
            pltpu.SemaphoreType.DMA((4,)),
            pltpu.SemaphoreType.DMA((6, 2)),
            pltpu.SemaphoreType.DMA((12,)),
            pltpu.SemaphoreType.DMA((2,)),
            pltpu.SemaphoreType.DMA,
            pltpu.SemaphoreType.DMA,
        ],
        compiler_params=pltpu.CompilerParams(collective_id=0, has_side_effects=True, vmem_limit_bytes=24 * 2**20),
    )(truss_k, *[pltpu.with_memory_space_constraint(v, pltpu.HBM) for v in (adj_diag, adj_right, alive_diag, alive_right)])


def solution(mesh):
    row = P("rows", None)
    return jax.shard_map(
        functools.partial(on_device, mesh.shape["rows"]),
        mesh=mesh,
        in_specs=(row, row, row, row, P()),
        out_specs=(row, P()),
        check_vma=False,
    )
```

```python
import functools

import jax
import jax.numpy as jnp
from jax import lax
from jax.experimental import pallas as pl
from jax.experimental.pallas import tpu as pltpu
from jax.sharding import PartitionSpec as P

F8 = jnp.float8_e4m3fn
F32 = jnp.float32
WORD = 32
ITERS = 3


def dot_nt(lhs, rhs):
    return lax.dot_general(lhs, rhs, (((1,), (1,)), ((), ())), preferred_element_type=F32)


def send(src, dst, send_sem, recv_sem, target):
    return pltpu.make_async_remote_copy(
        src_ref=src,
        dst_ref=dst,
        send_sem=send_sem,
        recv_sem=recv_sem,
        device_id=(target,),
        device_id_type=pl.DeviceIdType.MESH,
    )


def kernel(
    n, k_ref, ad_ref, ar_ref, ld_ref, lr_ref, out_ref, cnt_ref,
    k_smem, raw, own, halo, x, eye, tri, spare, psum_in, psum_next, psum_btw, mine, gathered,
    k_sem, raw_sems, send_sems, recv_sems, relay_sems, cnt_send, cnt_recv,
):
    t = ad_ref.shape[1]
    words = ad_ref.shape[0]
    me = lax.axis_index("rows")
    even = lax.rem(me, 2) == 0
    barrier = pltpu.get_barrier_semaphore()

    def greet(d, carry):
        pl.semaphore_signal(
            barrier, inc=1, device_id=(lax.rem(me + d, n),), device_id_type=pl.DeviceIdType.MESH
        )
        return carry

    lax.fori_loop(1, n, greet, 0)
    loads = [
        pltpu.make_async_copy(src, raw.at[i], raw_sems.at[i])
        for i, src in enumerate((ad_ref, ar_ref, ld_ref, lr_ref))
    ]
    for load in loads:
        load.start()
    k_load = pltpu.make_async_copy(k_ref, k_smem, k_sem)
    k_load.start()
    for load in loads:
        load.wait()
    own[0] = raw[0] & raw[2]
    own[1] = raw[1] & raw[3]

    AT, W, A = (pl.ds(i * t, t) for i in range(3))
    shift = lax.broadcasted_iota(jnp.int32, (WORD, t), 0)
    col = lax.broadcasted_iota(jnp.int32, (WORD, t), 1)

    half = t // 2

    def unpack(src, upper):
        for w in range(words):
            left = half if upper and 2 * w >= words else 0
            bits = (jnp.broadcast_to(src[w : w + 1, left:], (WORD, t - left)) >> shift[:, left:]) & 1
            if upper:
                bits = jnp.where(col[:, left:] - shift[:, left:] > WORD * w, bits, 0)
            yield pl.ds(WORD * w, WORD), pl.ds(left, t - left), bits.astype(F32).astype(F8)

    def put_across(src, j):
        for rows, _, bits in unpack(src, False):
            x[j, rows, A] = bits

    def put_transposed(j):
        x[j + 1, :, AT] = dot_nt(eye[...], x[j, :, A]).astype(F8)

    def put_within(src, j):
        for rows, cols, bits in unpack(src, True):
            tri[rows, cols] = bits
        flipped = dot_nt(eye[...], tri[...])
        x[j, :, W] = (flipped + tri[...].astype(F32)).astype(F8)

    row_id = lax.broadcasted_iota(jnp.int32, (t, t), 0)
    col_id = lax.broadcasted_iota(jnp.int32, (t, t), 1)
    eye[...] = jnp.where(row_id == col_id, 1.0, 0.0).astype(F32).astype(F8)
    tri[half:, :half] = jnp.zeros((t - half, half), F32).astype(F8)

    pl.semaphore_wait(barrier, n - 1)
    top, low = pl.ds(0, words // 2), pl.ds(words // 2, words // 2)
    whole, right = pl.ds(0, t), pl.ds(half, half)

    def pieces(source, slot, by, sends):
        parts = [(top, whole), (low, right if slot in (1, 3, 5) else whole)]
        return [
            send(
                source.at[rows, cols], halo.at[slot, rows, cols],
                sends.at[i], recv_sems.at[2 * slot + i], lax.rem(me + by + n, n),
            )
            for i, (rows, cols) in enumerate(parts)
        ]

    def start(slot):
        for piece in copies[slot]:
            piece.start()

    def arrive(slot):
        for piece in copies[slot]:
            piece.wait_recv()

    def left(copy):
        for piece in copy:
            piece.wait_send()

    routes = {2: (1, 1), 3: (0, -1), 1: (0, 1), 4: (1, -1), 0: (1, 2), 5: (0, -2)}
    copies = {
        slot: pieces(own.at[what], slot, by, send_sems.at[slot])
        for slot, (what, by) in routes.items()
    }
    to_right = pieces(halo.at[2], 0, 1, relay_sems)
    to_left = pieces(halo.at[3], 5, -1, relay_sems)
    start(3)
    start(2)

    @pl.when(even)
    def _():
        start(0)

    @pl.when(jnp.logical_not(even))
    def _():
        start(5)

    start(4)
    start(1)
    put_across(own.at[1], 1)

    k_load.wait()
    thresh = (k_smem[0] - 2).astype(F32)

    put_within(own.at[0], 1)
    put_transposed(1)
    psum_in[...] = dot_nt(x[1, :, t:], x[1, :, t:])
    psum_next[...] = dot_nt(x[2, :, AT], x[2, :, AT])
    psum_btw[...] = dot_nt(x[1, :, W], x[2, :, AT])

    def total(values):
        lanes = jnp.sum(values, axis=0, keepdims=True)
        return sum(lanes[:, i : i + 128] for i in range(0, t, 128))

    def keep(support, j, part):
        old = x[j, :, part].astype(F32)
        return old, jnp.where(support >= thresh, old, 0.0)

    def inside(j):
        return dot_nt(x[j], x[j])

    def between(j):
        return dot_nt(x[j, :, t:], x[j + 1, :, : 2 * t])

    counts = []

    def own_count(old_w, new_w, old_a, new_a):
        counts.append(total((old_w - new_w) + 2.0 * (old_a - new_a)))

    arrive(2)

    @pl.when(even)
    def _():
        for piece in to_right:
            piece.start()

    put_across(halo.at[2], 0)
    put_transposed(0)
    old_w, w0 = keep(psum_in[...] + dot_nt(x[1, :, AT], x[1, :, AT]), 1, W)
    arrive(1)
    put_within(halo.at[1], 0)
    _, am = keep(between(0), 0, A)
    arrive(3)

    @pl.when(jnp.logical_not(even))
    def _():
        for piece in to_left:
            piece.start()

    arrive(0)
    for rows, _, bits in unpack(halo.at[0], False):
        spare[rows, :] = bits
    x[0, :, AT] = dot_nt(eye[...], spare[...]).astype(F8)
    _, wm = keep(inside(0), 0, W)
    put_within(halo.at[3], 2)
    old_a, a0 = keep(psum_btw[...] + dot_nt(x[1, :, A], x[2, :, W]), 1, A)
    own_count(old_w, w0, old_a, a0)
    arrive(4)
    put_across(halo.at[4], 2)
    put_transposed(2)
    _, w1 = keep(psum_next[...] + dot_nt(x[2, :, t:], x[2, :, t:]), 2, W)
    arrive(5)
    put_within(halo.at[5], 3)
    _, a1 = keep(between(2), 2, A)
    x[0, :, W] = wm.astype(F8)
    x[0, :, A] = am.astype(F8)
    x[1, :, W] = w0.astype(F8)
    x[1, :, A] = a0.astype(F8)
    x[2, :, W] = w1.astype(F8)
    x[2, :, A] = a1.astype(F8)
    put_transposed(0)
    put_transposed(1)

    _, am = keep(between(0), 0, A)
    old_w, w0 = keep(inside(1), 1, W)
    old_a, a0 = keep(between(1), 1, A)
    own_count(old_w, w0, old_a, a0)
    _, w1 = keep(inside(2), 2, W)
    x[0, :, A] = am.astype(F8)
    x[1, :, W] = w0.astype(F8)
    x[1, :, A] = a0.astype(F8)
    x[2, :, W] = w1.astype(F8)
    put_transposed(0)
    put_transposed(1)

    support_w = inside(1)
    old_w, w0 = keep(support_w, 1, W)
    support_a = between(1)
    old_a, a0 = keep(support_a, 1, A)
    own_count(old_w, w0, old_a, a0)
    lane = lax.broadcasted_iota(jnp.int32, (1, 128), 1)
    packed = jnp.zeros((1, 128), F32)
    for step, row in enumerate(counts):
        packed = jnp.where(lane == step, jnp.sum(row, axis=1, keepdims=True), packed)
    mine[...] = packed.astype(jnp.int32)

    def share(d, carry):
        send(mine, gathered.at[d - 1], cnt_send, cnt_recv, lax.rem(me + d, n)).start()
        return carry

    lax.fori_loop(1, n, share, 0)
    out_ref[:, :t] = support_w * w0
    out_ref[:, t:] = support_a * a0
    for slot in range(1, 5):
        left(copies[slot])

    @pl.when(even)
    def _():
        left(copies[0])
        left(to_right)

    @pl.when(jnp.logical_not(even))
    def _():
        left(copies[5])
        left(to_left)

    pltpu.make_async_copy(gathered, gathered, cnt_recv).wait()
    cnt_ref[: n - 1] = gathered[...]
    cnt_ref[n - 1] = mine[...]
    pltpu.make_async_copy(gathered, gathered, cnt_send).wait()


def finish(support_ref, cnt_ref, out_ref, removed_ref, sems):
    parts = sems.shape[0]
    rows = support_ref.shape[0] // parts
    copies = [
        pltpu.make_async_copy(
            support_ref.at[pl.ds(i * rows, rows)], out_ref.at[pl.ds(i * rows, rows)], sems.at[i]
        )
        for i in range(parts)
    ]
    for copy in copies:
        copy.start()
    summed = jnp.sum(cnt_ref[...], axis=0)
    lane = lax.broadcasted_iota(jnp.int32, summed.shape, 1)
    for step in range(removed_ref.shape[0]):
        removed_ref[step] = jnp.sum(jnp.where(lane == step, summed, 0)) // 2
    for copy in copies:
        copy.wait()


def on_device(n, adj_diag, adj_right, alive_diag, alive_right, truss_k):
    words, t = adj_diag.shape
    vmem = pl.BlockSpec(memory_space=pltpu.VMEM)
    smem = pl.BlockSpec(memory_space=pltpu.SMEM)
    hbm = pl.BlockSpec(memory_space=pltpu.HBM)
    args = [
        pltpu.with_memory_space_constraint(v, pltpu.HBM)
        for v in (adj_diag, adj_right, alive_diag, alive_right)
    ]
    support, counts = pl.pallas_call(
        functools.partial(kernel, n),
        out_shape=(
            jax.ShapeDtypeStruct((t, 2 * t), F32),
            jax.ShapeDtypeStruct((n, 1, 128), jnp.int32),
        ),
        in_specs=[hbm] * 5,
        out_specs=(vmem, vmem),
        scratch_shapes=[
            pltpu.SMEM((1,), jnp.int32),
            pltpu.VMEM((4, words, t), jnp.int32),
            pltpu.VMEM((2, words, t), jnp.int32),
            pltpu.VMEM((6, words, t), jnp.int32),
            pltpu.VMEM((4, t, 3 * t), F8),
            pltpu.VMEM((t, t), F8),
            pltpu.VMEM((t, t), F8),
            pltpu.VMEM((t, t), F8),
            pltpu.VMEM((t, t), F32),
            pltpu.VMEM((t, t), F32),
            pltpu.VMEM((t, t), F32),
            pltpu.VMEM((1, 128), jnp.int32),
            pltpu.VMEM((n - 1, 1, 128), jnp.int32),
            pltpu.SemaphoreType.DMA,
            pltpu.SemaphoreType.DMA((4,)),
            pltpu.SemaphoreType.DMA((6, 2)),
            pltpu.SemaphoreType.DMA((12,)),
            pltpu.SemaphoreType.DMA((2,)),
            pltpu.SemaphoreType.DMA,
            pltpu.SemaphoreType.DMA,
        ],
        compiler_params=pltpu.CompilerParams(collective_id=0, has_side_effects=True, vmem_limit_bytes=24 * 2**20),
    )(truss_k, *args)
    return pl.pallas_call(
        finish,
        out_shape=(
            jax.ShapeDtypeStruct((t, 2 * t), F32),
            jax.ShapeDtypeStruct((ITERS,), jnp.int32),
        ),
        in_specs=[vmem, vmem],
        out_specs=(hbm, smem),
        scratch_shapes=[pltpu.SemaphoreType.DMA((4,))],
        compiler_params=pltpu.CompilerParams(vmem_limit_bytes=2**20),
    )(support, counts)


def solution(mesh):
    row = P("rows", None)
    return jax.shard_map(
        functools.partial(on_device, mesh.shape["rows"]),
        mesh=mesh,
        in_specs=(row, row, row, row, P()),
        out_specs=(row, P()),
        check_vma=False,
    )
```

```python
import functools

import jax
import jax.numpy as jnp
from jax import lax
from jax.experimental import pallas as pl
from jax.experimental.pallas import tpu as pltpu
from jax.sharding import PartitionSpec as P

F8 = jnp.float8_e4m3fn
F32 = jnp.float32
WORD = 32
ITERS = 3


def dot_nt(lhs, rhs):
    return lax.dot_general(lhs, rhs, (((1,), (1,)), ((), ())), preferred_element_type=F32)


def send(src, dst, send_sem, recv_sem, target):
    return pltpu.make_async_remote_copy(
        src_ref=src,
        dst_ref=dst,
        send_sem=send_sem,
        recv_sem=recv_sem,
        device_id=(target,),
        device_id_type=pl.DeviceIdType.MESH,
    )


def kernel(
    n, k_ref, ad_ref, ar_ref, ld_ref, lr_ref, out_ref, cnt_ref,
    k_smem, raw, own, halo, x, eye, tri, spare, psum_in, psum_next, psum_btw, mine, gathered,
    k_sem, raw_sems, send_sems, recv_sems, relay_sems, cnt_send, cnt_recv,
):
    t = ad_ref.shape[1]
    words = ad_ref.shape[0]
    me = lax.axis_index("rows")
    even = lax.rem(me, 2) == 0
    barrier = pltpu.get_barrier_semaphore()

    def greet(d, carry):
        pl.semaphore_signal(
            barrier, inc=1, device_id=(lax.rem(me + d, n),), device_id_type=pl.DeviceIdType.MESH
        )
        return carry

    for d in (1, n - 1, 2, n - 2):
        greet(d, 0)
    loads = [
        pltpu.make_async_copy(src, raw.at[i], raw_sems.at[i])
        for i, src in enumerate((ad_ref, ar_ref, ld_ref, lr_ref))
    ]
    for load in loads:
        load.start()
    k_load = pltpu.make_async_copy(k_ref, k_smem, k_sem)
    k_load.start()
    lax.fori_loop(3, n - 2, greet, 0)
    for load in loads:
        load.wait()
    own[0] = raw[0] & raw[2]
    own[1] = raw[1] & raw[3]

    AT, W, A = (pl.ds(i * t, t) for i in range(3))
    shift = lax.broadcasted_iota(jnp.int32, (WORD, t), 0)
    col = lax.broadcasted_iota(jnp.int32, (WORD, t), 1)

    half = t // 2

    def unpack(src, upper):
        for w in range(words):
            left = half if upper and 2 * w >= words else 0
            bits = (jnp.broadcast_to(src[w : w + 1, left:], (WORD, t - left)) >> shift[:, left:]) & 1
            if upper:
                bits = jnp.where(col[:, left:] - shift[:, left:] > WORD * w, bits, 0)
            yield pl.ds(WORD * w, WORD), pl.ds(left, t - left), bits.astype(F32).astype(F8)

    def put_across(src, j):
        for rows, _, bits in unpack(src, False):
            x[j, rows, A] = bits

    def put_transposed(j):
        x[j + 1, :, AT] = dot_nt(eye[...], x[j, :, A]).astype(F8)

    def put_within(src, j):
        for rows, cols, bits in unpack(src, True):
            tri[rows, cols] = bits
        flipped = dot_nt(eye[...], tri[...])
        x[j, :, W] = (flipped + tri[...].astype(F32)).astype(F8)

    row_id = lax.broadcasted_iota(jnp.int32, (t, t), 0)
    col_id = lax.broadcasted_iota(jnp.int32, (t, t), 1)
    eye[...] = jnp.where(row_id == col_id, 1.0, 0.0).astype(F32).astype(F8)
    tri[half:, :half] = jnp.zeros((t - half, half), F32).astype(F8)

    pl.semaphore_wait(barrier, n - 1)
    top, low = pl.ds(0, words // 2), pl.ds(words // 2, words // 2)
    whole, right = pl.ds(0, t), pl.ds(half, half)

    def pieces(source, slot, by, sends):
        parts = [(top, whole), (low, right if slot in (1, 3, 5) else whole)]
        return [
            send(
                source.at[rows, cols], halo.at[slot, rows, cols],
                sends.at[i], recv_sems.at[2 * slot + i], lax.rem(me + by + n, n),
            )
            for i, (rows, cols) in enumerate(parts)
        ]

    def start(slot):
        for piece in copies[slot]:
            piece.start()

    def arrive(slot):
        for piece in copies[slot]:
            piece.wait_recv()

    def left(copy):
        for piece in copy:
            piece.wait_send()

    routes = {2: (1, 1), 3: (0, -1), 1: (0, 1), 4: (1, -1), 0: (1, 2), 5: (0, -2)}
    copies = {
        slot: pieces(own.at[what], slot, by, send_sems.at[slot])
        for slot, (what, by) in routes.items()
    }
    to_right = pieces(halo.at[2], 0, 1, relay_sems)
    to_left = pieces(halo.at[3], 5, -1, relay_sems)
    start(3)
    start(2)

    @pl.when(even)
    def _():
        start(0)

    @pl.when(jnp.logical_not(even))
    def _():
        start(5)

    start(4)
    start(1)
    put_across(own.at[1], 1)

    k_load.wait()
    thresh = (k_smem[0] - 2).astype(F32)

    put_within(own.at[0], 1)
    put_transposed(1)
    psum_in[...] = dot_nt(x[1, :, t:], x[1, :, t:])
    psum_next[...] = dot_nt(x[2, :, AT], x[2, :, AT])
    psum_btw[...] = dot_nt(x[1, :, W], x[2, :, AT])

    def total(values):
        lanes = jnp.sum(values, axis=0, keepdims=True)
        return sum(lanes[:, i : i + 128] for i in range(0, t, 128))

    def keep(support, j, part):
        old = x[j, :, part].astype(F32)
        return old, jnp.where(support >= thresh, old, 0.0)

    def inside(j):
        return dot_nt(x[j], x[j])

    def between(j):
        return dot_nt(x[j, :, t:], x[j + 1, :, : 2 * t])

    def between_plain(j):
        return jnp.dot(x[j, :, A], x[j + 1, :, W], preferred_element_type=F32) + jnp.dot(
            x[j, :, W], x[j, :, A], preferred_element_type=F32
        )

    counts = []

    def own_count(old_w, new_w, old_a, new_a):
        counts.append(total((old_w - new_w) + 2.0 * (old_a - new_a)))

    arrive(2)

    @pl.when(even)
    def _():
        for piece in to_right:
            piece.start()

    put_across(halo.at[2], 0)
    put_transposed(0)
    old_w, w0 = keep(psum_in[...] + dot_nt(x[1, :, AT], x[1, :, AT]), 1, W)
    arrive(1)
    put_within(halo.at[1], 0)
    _, am = keep(between(0), 0, A)
    arrive(0)
    for rows, _, bits in unpack(halo.at[0], False):
        spare[rows, :] = bits
    x[0, :, AT] = dot_nt(eye[...], spare[...]).astype(F8)
    _, wm = keep(inside(0), 0, W)
    x[0, :, W] = wm.astype(F8)
    x[0, :, A] = am.astype(F8)
    x[1, :, W] = w0.astype(F8)
    put_transposed(0)
    arrive(3)

    @pl.when(jnp.logical_not(even))
    def _():
        for piece in to_left:
            piece.start()

    put_within(halo.at[3], 2)
    old_a, a0 = keep(psum_btw[...] + dot_nt(x[1, :, A], x[2, :, W]), 1, A)
    own_count(old_w, w0, old_a, a0)
    arrive(4)
    put_across(halo.at[4], 2)
    _, w1 = keep(psum_next[...] + dot_nt(x[2, :, t:], x[2, :, t:]), 2, W)
    arrive(5)
    put_within(halo.at[5], 3)
    _, a1 = keep(between_plain(2), 2, A)
    x[1, :, A] = a0.astype(F8)
    x[2, :, W] = w1.astype(F8)
    x[2, :, A] = a1.astype(F8)
    put_transposed(1)

    _, am = keep(between(0), 0, A)
    old_w, w0 = keep(inside(1), 1, W)
    old_a, a0 = keep(between(1), 1, A)
    own_count(old_w, w0, old_a, a0)
    _, w1 = keep(inside(2), 2, W)
    x[0, :, A] = am.astype(F8)
    x[1, :, W] = w0.astype(F8)
    x[1, :, A] = a0.astype(F8)
    x[2, :, W] = w1.astype(F8)
    put_transposed(0)

    support_w = inside(1)
    old_w, w0 = keep(support_w, 1, W)
    support_a = between_plain(1)
    old_a, a0 = keep(support_a, 1, A)
    own_count(old_w, w0, old_a, a0)
    lane = lax.broadcasted_iota(jnp.int32, (1, 128), 1)
    packed = jnp.zeros((1, 128), F32)
    for step, row in enumerate(counts):
        packed = jnp.where(lane == step, jnp.sum(row, axis=1, keepdims=True), packed)
    mine[...] = packed.astype(jnp.int32)

    def share(d, carry):
        send(mine, gathered.at[d - 1], cnt_send, cnt_recv, lax.rem(me + d, n)).start()
        return carry

    lax.fori_loop(1, n, share, 0)
    out_ref[:, :t] = support_w * w0
    out_ref[:, t:] = support_a * a0
    for slot in range(1, 5):
        left(copies[slot])

    @pl.when(even)
    def _():
        left(copies[0])
        left(to_right)

    @pl.when(jnp.logical_not(even))
    def _():
        left(copies[5])
        left(to_left)

    pltpu.make_async_copy(gathered, gathered, cnt_recv).wait()
    cnt_ref[: n - 1] = gathered[...]
    cnt_ref[n - 1] = mine[...]
    pltpu.make_async_copy(gathered, gathered, cnt_send).wait()


def finish(support_ref, cnt_ref, out_ref, removed_ref, sems):
    parts = sems.shape[0]
    rows = support_ref.shape[0] // parts
    copies = [
        pltpu.make_async_copy(
            support_ref.at[pl.ds(i * rows, rows)], out_ref.at[pl.ds(i * rows, rows)], sems.at[i]
        )
        for i in range(parts)
    ]
    for copy in copies:
        copy.start()
    summed = jnp.sum(cnt_ref[...], axis=0)
    lane = lax.broadcasted_iota(jnp.int32, summed.shape, 1)
    for step in range(removed_ref.shape[0]):
        removed_ref[step] = jnp.sum(jnp.where(lane == step, summed, 0)) // 2
    for copy in copies:
        copy.wait()


def on_device(n, adj_diag, adj_right, alive_diag, alive_right, truss_k):
    words, t = adj_diag.shape
    vmem = pl.BlockSpec(memory_space=pltpu.VMEM)
    smem = pl.BlockSpec(memory_space=pltpu.SMEM)
    hbm = pl.BlockSpec(memory_space=pltpu.HBM)
    args = [
        pltpu.with_memory_space_constraint(v, pltpu.HBM)
        for v in (adj_diag, adj_right, alive_diag, alive_right)
    ]
    support, counts = pl.pallas_call(
        functools.partial(kernel, n),
        out_shape=(
            jax.ShapeDtypeStruct((t, 2 * t), F32),
            jax.ShapeDtypeStruct((n, 1, 128), jnp.int32),
        ),
        in_specs=[hbm] * 5,
        out_specs=(vmem, vmem),
        scratch_shapes=[
            pltpu.SMEM((1,), jnp.int32),
            pltpu.VMEM((4, words, t), jnp.int32),
            pltpu.VMEM((2, words, t), jnp.int32),
            pltpu.VMEM((6, words, t), jnp.int32),
            pltpu.VMEM((4, t, 3 * t), F8),
            pltpu.VMEM((t, t), F8),
            pltpu.VMEM((t, t), F8),
            pltpu.VMEM((t, t), F8),
            pltpu.VMEM((t, t), F32),
            pltpu.VMEM((t, t), F32),
            pltpu.VMEM((t, t), F32),
            pltpu.VMEM((1, 128), jnp.int32),
            pltpu.VMEM((n - 1, 1, 128), jnp.int32),
            pltpu.SemaphoreType.DMA,
            pltpu.SemaphoreType.DMA((4,)),
            pltpu.SemaphoreType.DMA((6, 2)),
            pltpu.SemaphoreType.DMA((12,)),
            pltpu.SemaphoreType.DMA((2,)),
            pltpu.SemaphoreType.DMA,
            pltpu.SemaphoreType.DMA,
        ],
        compiler_params=pltpu.CompilerParams(collective_id=0, has_side_effects=True, vmem_limit_bytes=24 * 2**20),
    )(truss_k, *args)
    return pl.pallas_call(
        finish,
        out_shape=(
            jax.ShapeDtypeStruct((t, 2 * t), F32),
            jax.ShapeDtypeStruct((ITERS,), jnp.int32),
        ),
        in_specs=[vmem, vmem],
        out_specs=(hbm, smem),
        scratch_shapes=[pltpu.SemaphoreType.DMA((4,))],
        compiler_params=pltpu.CompilerParams(vmem_limit_bytes=2**20),
    )(support, counts)


def solution(mesh):
    row = P("rows", None)
    return jax.shard_map(
        functools.partial(on_device, mesh.shape["rows"]),
        mesh=mesh,
        in_specs=(row, row, row, row, P()),
        out_specs=(row, P()),
        check_vma=False,
    )
```
